32 devices in a mesh: fsdp: 8 (over z, y), rep: 4 (over x, core).
Axes of the slice: x: 2, y: 2, z: 4, core: 2. Of those that a mesh axis runs over, the one named last changes fastest.
Arguments:
- partial_grad: bfloat16 [4, 8, 1024, 1024], P('rep', None, 'fsdp'), may hold values from -3 to 3
- owner_table: int32 [8, 2], replicated, may hold values from -1 to 7, as said below
- left_stat: float32 [8, 2, 1024, 1024], P('fsdp', None, None, 'rep'), may hold values from -6 to 6
- right_stat: float32 [8, 2, 1024, 1024], P('fsdp', None, None, 'rep'), may hold values from -6 to 6
- left_root: bfloat16 [8, 2, 1024, 1024], P('fsdp', None, None, 'rep'), may hold values from -0.1875 to 0.1875
- right_root: bfloat16 [8, 2, 1024, 1024], P('fsdp', None, None, 'rep'), may hold values from -0.1875 to 0.1875
Outputs:
- left_new: float32 [8, 2, 1024, 1024], P('fsdp', None, None, 'rep')
- right_new: float32 [8, 2, 1024, 1024], P('fsdp', None, None, 'rep')
- update: bfloat16 [8, 1024, 1024], P(None, 'fsdp', 'rep')
The draws below stay inside these ranges and needn't reach their ends.
Inputs may be any that keep to these rules, and one draw needn't show every extreme that they name: `owner_table`: each of the 8 blocks stands in exactly one slot and -1 marks an empty slot; some owner fills all 2 slots and some owner has none.
All inputs are finite; a program needn't handle non-finite values.
Results may differ from the reference program's by a relative error of at most 0.014.
Values may be sent and summed in bfloat16 or wider, within the bound.
No kernel may reach another device: no remote copies, remote signals or barrier semaphores. Data moves between devices by JAX's collectives and lax.ppermute only.
A program may use at most 64 MiB of HBM per device.

```python
import jax
import jax.numpy as jnp
from jax import lax

BS = 1024
SLOTS = 2
BLOCKS = 8
N_FSDP = 8
N_REP = 4


def draw_owner_table(key, part):
    owners = BLOCKS
    first_key, second_key, third_key = jax.random.split(jax.random.fold_in(key, 7), 3)
    order = jax.random.permutation(first_key, owners).astype(jnp.int32)
    ranking = jnp.zeros((owners,), jnp.int32).at[order].set(jnp.arange(owners, dtype=jnp.int32))
    doubled = jax.random.randint(second_key, (), max(1, owners // 4), owners // 2 + 1).astype(jnp.int32)
    loads = jnp.where(ranking < doubled, 2, jnp.where(ranking < 2 * doubled, 0, 1)).astype(jnp.int32)
    filled = jnp.stack([loads >= 1, loads >= 2], axis=1).reshape(-1)
    counter = jnp.cumsum(filled.astype(jnp.int32)) - 1
    shuffled = jax.random.permutation(third_key, owners).astype(jnp.int32)
    picked = jnp.take(shuffled, jnp.maximum(counter, 0))
    return jnp.where(filled, picked, -1).astype(jnp.int32).reshape(owners, SLOTS)


def shard_levels(key, shape, cuts, least, largest):
    factor_of, own = 1.0, jax.random.fold_in(key, 6)
    for axis_at, blocks in cuts:
        heights = jnp.exp(jax.random.uniform(jax.random.fold_in(own, axis_at), (blocks,), jnp.float32, least / len(cuts), largest / len(cuts)))
        factor_of = factor_of * jnp.repeat(heights, shape[axis_at] // blocks).reshape([-1 if axis == axis_at else 1 for axis in range(len(shape))])
    return factor_of


def noise(own_key, dims, deviation, limit, pieces=(), kind=jnp.bfloat16):
    values = deviation * jax.random.normal(own_key, dims, jnp.float32)
    if pieces:
        values = values * shard_levels(own_key, dims, pieces, -0.22, 0.18)
    return jnp.clip(values, -limit, limit).astype(kind)


def setup_inputs(seed: int = 0) -> dict:
    key_of = jax.random.split(jax.random.key(seed), 7)
    return {
        "partial_grad": noise(key_of[0], (N_REP, BLOCKS, BS, BS), 0.5, 3.0, ((0, 4), (2, 8))),
        "owner_table": draw_owner_table(jax.random.fold_in(key_of[6], 71), 0),
        "left_stat": noise(key_of[2], (N_FSDP, SLOTS, BS, BS), 1.0, 6.0, ((0, 8), (3, 4)), jnp.float32),
        "right_stat": noise(key_of[3], (N_FSDP, SLOTS, BS, BS), 1.0, 6.0, ((0, 8), (3, 4)), jnp.float32),
        "left_root": noise(key_of[4], (N_FSDP, SLOTS, BS, BS), BS ** -0.5, 0.1875, ((0, 8), (3, 4))),
        "right_root": noise(key_of[5], (N_FSDP, SLOTS, BS, BS), BS ** -0.5, 0.1875, ((0, 8), (3, 4))),
    }


decay_rate = 0.99


def one_slot(summed, inputs):
    block_index, is_filled, left_old, right_old, left_inv, right_inv = inputs
    picked = lax.dynamic_index_in_dim(summed, block_index, 0, keepdims=False)
    slot_grad = jnp.where(is_filled, picked, jnp.zeros((), jnp.bfloat16))
    left_term = jnp.dot(slot_grad, slot_grad.T, preferred_element_type=jnp.float32)
    right_term = jnp.dot(slot_grad.T, slot_grad, preferred_element_type=jnp.float32)
    left_next = jnp.where(is_filled, decay_rate * left_old + (1.0 - decay_rate) * left_term, left_old)
    right_next = jnp.where(is_filled, decay_rate * right_old + (1.0 - decay_rate) * right_term, right_old)
    applied = jnp.dot(left_inv, slot_grad, preferred_element_type=jnp.float32).astype(jnp.bfloat16)
    result = jnp.dot(applied, right_inv, preferred_element_type=jnp.float32).astype(jnp.bfloat16)
    return left_next, right_next, result


def reference(partial_grad, owner_table, left_stat, right_stat, left_root, right_root):
    summed = jnp.sum(partial_grad.astype(jnp.float32), axis=0).astype(jnp.bfloat16)
    flat_table = owner_table.reshape(-1)
    filled_flat = flat_table >= 0
    index_flat = jnp.maximum(flat_table, 0).astype(jnp.int32)
    order = BS
    stacked = (index_flat, filled_flat, left_stat.reshape(-1, order, order), right_stat.reshape(-1, order, order), left_root.reshape(-1, order, order), right_root.reshape(-1, order, order))
    left_all, right_all, result_all = lax.map(lambda inputs: one_slot(summed, inputs), stacked)
    slot_ids = jnp.arange(flat_table.shape[0], dtype=jnp.int32)
    block_ids = jnp.arange(BLOCKS, dtype=jnp.int32)
    positions = jnp.sum(jnp.where(flat_table[None, :] == block_ids[:, None], slot_ids[None, :], 0), axis=1).astype(jnp.int32)
    update = jnp.take(result_all, positions, axis=0)
    return left_all.reshape(left_stat.shape), right_all.reshape(right_stat.shape), update
```

```python
import functools

import jax
import jax.numpy as jnp
from jax import lax
from jax.experimental import pallas as pl
from jax.experimental.pallas import tpu as pltpu
from jax.sharding import PartitionSpec as P

decay_rate = 0.99


def route_kernel(owners, table_ref, me_ref, mine_ref, core_ref, across_ref, *pieces):
    slots = pieces[0].shape[0]
    for k in range(owners):
        owner = lax.rem(me_ref[0] + k, owners)
        for s in range(slots):
            block = table_ref[owner * slots + s]

            @pl.when(block >= 0)
            def _(k=k, s=s, block=block):
                total = mine_ref[block].astype(jnp.float32) + core_ref[block].astype(jnp.float32)
                pieces[k][s] = (total + across_ref[block].astype(jnp.float32)).astype(jnp.bfloat16)

            @pl.when(block < 0)
            def _(k=k, s=s):
                pieces[k][s] = jnp.zeros(pieces[k].shape[1:], jnp.bfloat16)


def apply_kernel(owners, quarters, me_ref, *refs):
    count = owners * quarters
    pieces, left = refs[:count], refs[count : count + quarters]
    right_ref, grad_ref = refs[count + quarters], refs[count + quarters + 1]
    outs, prod_ref = refs[count + quarters + 2 : -1], refs[-1]
    slots, rows, width = pieces[0].shape
    me, rep = me_ref[0], me_ref[1]
    for k in range(owners):
        first = pl.multiple_of(lax.rem(me - k + owners, owners) * rows, rows)
        for q in range(quarters):
            col = pl.multiple_of((rep ^ q) * width, width)
            grad_ref[:, pl.ds(first, rows), pl.ds(col, width)] = pieces[k * quarters + q][...]
    for s in range(slots):
        prod_ref[s] = jnp.dot(
            grad_ref[s], right_ref[s], preferred_element_type=jnp.float32
        ).astype(jnp.bfloat16)
    for k in range(owners):
        first = pl.multiple_of(lax.rem(me + k, owners) * rows, rows)
        for s in range(slots):
            total = None
            for q in range(quarters):
                band = pl.ds(pl.multiple_of((rep ^ q) * width, width), width)
                term = jnp.dot(
                    left[q][s, pl.ds(first, rows), :],
                    prod_ref[s, band, :],
                    preferred_element_type=jnp.float32,
                )
                total = term if total is None else total + term
            outs[k][s] = total.astype(jnp.bfloat16)


def collect_kernel(owners, table_ref, me_ref, *refs):
    pieces, out_ref = refs[:-1], refs[-1]
    slots = pieces[0].shape[0]
    for k in range(owners):
        owner = lax.rem(me_ref[0] - k + owners, owners)
        for s in range(slots):
            block = table_ref[owner * slots + s]

            @pl.when(block >= 0)
            def _(k=k, s=s, block=block):
                out_ref[block] = pieces[k][s]


def call(kernel, scalars, out_shape, ins, scratch=()):
    vmem = pl.BlockSpec(memory_space=pltpu.VMEM)
    smem = pl.BlockSpec(memory_space=pltpu.SMEM)
    return pl.pallas_call(
        kernel,
        out_shape=out_shape,
        in_specs=[smem] * len(scalars) + [vmem] * len(ins),
        out_specs=jax.tree.map(lambda _: vmem, out_shape),
        scratch_shapes=scratch,
        compiler_params=pltpu.CompilerParams(vmem_limit_bytes=32 * 1024 * 1024),
    )(*scalars, *ins)


def on_device(owners, quarters, partial_grad, owner_table, left_stat, right_stat, left_root, right_root):
    grad = partial_grad[0]
    me, rep = lax.axis_index("fsdp"), lax.axis_index("rep")
    slots, order, width = left_stat.shape[1:]
    rows = grad.shape[1]
    table = owner_table.reshape(-1)
    where = jnp.stack([me, rep]).astype(jnp.int32)

    def swap(x, bits):
        return lax.ppermute(x, "rep", [(r, r ^ bits) for r in range(quarters)])

    def shift(x, k):
        return lax.ppermute(x, "fsdp", [(f, (f + k) % owners) for f in range(owners)])

    def cut(q):
        return lax.dynamic_slice_in_dim(grad, q * width, width, 2)

    def add(a, b):
        return (a.astype(jnp.float32) + b.astype(jnp.float32)).astype(jnp.bfloat16)

    first = swap(cut(rep ^ 3), 1)
    second = swap(cut(rep ^ 1), 1)
    across = swap(add(cut(rep ^ 2), first), 2)
    piece = jax.ShapeDtypeStruct((slots, rows, width), jnp.bfloat16)
    pieces = call(
        functools.partial(route_kernel, owners),
        (table, where),
        (piece,) * owners,
        (cut(rep), second, across),
    )
    left = left_root[0]
    far = swap(left, 2)
    left_quarters = [left, swap(left, 1), far, swap(far, 1)]
    gathered = []
    for k in range(owners):
        mine = pieces[k] if k == 0 else shift(pieces[k], k)
        far = swap(mine, 2)
        gathered += [mine, swap(mine, 1), far, swap(far, 1)]
    results = call(
        functools.partial(apply_kernel, owners, quarters),
        (where,),
        (jax.ShapeDtypeStruct((slots, order, order), jnp.bfloat16),) + (piece,) * owners,
        (*gathered, *left_quarters, right_root[0]),
        (pltpu.VMEM((slots, order, width), jnp.bfloat16),),
    )
    gradient, results = results[0], results[1:]
    returned = [results[0]] + [shift(results[k], k) for k in range(1, owners)]
    update = call(
        functools.partial(collect_kernel, owners),
        (table, where),
        jax.ShapeDtypeStruct((grad.shape[0], rows, width), jnp.bfloat16),
        tuple(returned),
    )
    keeper = (lax.dynamic_index_in_dim(owner_table, me, 0, keepdims=False) >= 0)[:, None, None]
    rows_share = lax.dynamic_slice_in_dim(gradient, rep * width, width, 1)
    cols_share = lax.dynamic_slice_in_dim(gradient, rep * width, width, 2)
    left_term = jnp.einsum("sik,sjk->sij", gradient, rows_share, preferred_element_type=jnp.float32)
    right_term = jnp.einsum("ski,skj->sij", gradient, cols_share, preferred_element_type=jnp.float32)
    left_next = jnp.where(keeper, decay_rate * left_stat[0] + (1.0 - decay_rate) * left_term, left_stat[0])
    right_next = jnp.where(keeper, decay_rate * right_stat[0] + (1.0 - decay_rate) * right_term, right_stat[0])
    return left_next[None], right_next[None], update


def solution(mesh):
    owners, quarters = mesh.shape["fsdp"], mesh.shape["rep"]
    assert quarters == 4
    stat = P("fsdp", None, None, "rep")
    return jax.shard_map(
        functools.partial(on_device, owners, quarters),
        mesh=mesh,
        in_specs=(P("rep", None, "fsdp", None), P(), stat, stat, stat, stat),
        out_specs=(stat, stat, P(None, "fsdp", "rep")),
        check_vma=False,
    )
```

```python
import functools

import jax
import jax.numpy as jnp
from jax import lax
from jax.experimental import pallas as pl
from jax.experimental.pallas import tpu as pltpu
from jax.sharding import PartitionSpec as P


decay_rate = 0.99


def pair_kernel(where_ref, mine_ref, near_ref, *outs):
    width = mine_ref.shape[2]
    cols = pl.ds(pl.multiple_of((where_ref[1] ^ 2) * width, width), width)
    total = (mine_ref[...].astype(jnp.float32) + near_ref[:, :, cols].astype(jnp.float32)).astype(jnp.bfloat16)
    for p in range(2):
        outs[p][...] = total[:, :, p * width // 2 : (p + 1) * width // 2]


def base_kernel(where_ref, grad_ref, near_ref, out_ref):
    width = out_ref.shape[3]
    for q in range(2):
        cols = pl.ds(pl.multiple_of((where_ref[1] ^ q) * width, width), width)
        out_ref[q] = grad_ref[:, :, cols].astype(jnp.float32) + near_ref[:, :, cols].astype(jnp.float32)


def route_kernel(wanted, table_ref, where_ref, base_ref, *refs):
    sums, pieces = refs[: len(refs) - len(wanted)], refs[len(refs) - len(wanted) :]
    me, side = where_ref[0], where_ref[1] & 1
    step = sums[0].shape[2]
    for (k, parts), piece in zip(wanted, pieces):
        block = table_ref[(me ^ k) * 2 + side]

        @pl.when(block >= 0)
        def _(parts=parts, piece=piece, block=block):
            for n, p in enumerate(parts):
                for q in range(2):
                    total = base_ref[q, block, :, p * step : (p + 1) * step]
                    far_ref = sums[2 * p + q] if len(sums) > 2 else sums[q]
                    total = total + far_ref[block].astype(jnp.float32)
                    piece[side ^ q, :, n * step : (n + 1) * step] = total.astype(jnp.bfloat16)

        @pl.when(block < 0)
        def _(piece=piece):
            piece[...] = jnp.zeros(piece.shape, jnp.bfloat16)


def join_kernel(*refs):
    for n in range(len(refs) - 1):
        refs[-1][n] = refs[n][...]


def product_kernel(owners, where_ref, *refs):
    joined_ref, right_ref, beside_ref, grad_ref, prod_ref = refs[-5:]
    half = owners // 2
    rows, width = refs[0].shape[1:]
    step = width // 2
    me, side, place = where_ref[0], where_ref[1] & 1, where_ref[1] >> 1
    for k in range(owners):
        first = pl.ds(pl.multiple_of((me ^ k) * rows, rows), rows)
        for i in range(2):
            for q in range(2):
                col = pl.multiple_of(((place ^ i) * 2 + q) * width, width)
                if k < half:
                    grad_ref[first, pl.ds(col, width)] = refs[2 * k + i][q]
                else:
                    early = joined_ref[k - half, q] if i else refs[2 * owners + k - half][q]
                    grad_ref[first, pl.ds(col, step)] = early
                    grad_ref[first, pl.ds(pl.multiple_of(col + step, step), step)] = refs[2 * k + i][q]
    for i, right in enumerate((right_ref[side], beside_ref[...])):
        prod_ref[i] = jnp.dot(grad_ref[...], right, preferred_element_type=jnp.float32).astype(jnp.bfloat16)


def apply_kernel(where_ref, near_ref, far_ref, prod_ref, even_ref, odd_ref):
    _, both, width = near_ref.shape
    rows = both // 2
    me, rep = where_ref[0], where_ref[1]
    side = rep & 1
    swapped = (me & 1) == 1
    for i in range(2):
        total = None
        for q in range(4):
            band = pl.ds(pl.multiple_of((rep ^ q) * width, width), width)
            ref = far_ref if q & 2 else near_ref
            term = jnp.dot(ref[q & 1], prod_ref[i, band, :], preferred_element_type=jnp.float32)
            total = term if total is None else total + term
        total = total.astype(jnp.bfloat16)
        even_ref[side ^ i] = jnp.where(swapped, total[rows:], total[:rows])
        odd_ref[side ^ i] = jnp.where(swapped, total[:rows], total[rows:])


def stats_kernel(table_ref, where_ref, grad_ref, other_ref, left_ref, right_ref, left_out, right_out):
    me, rep = where_ref[0], where_ref[1]
    _, _, width = left_ref.shape
    slot = pl.program_id(0)
    filled = table_ref[me * 2 + slot] >= 0
    share = pl.ds(pl.multiple_of(rep * width, width), width)

    def update(ref):
        rows, cols = ref[share, :], ref[:, share]
        left = lax.dot_general(ref[...], rows, (((1,), (1,)), ((), ())), preferred_element_type=jnp.float32)
        left_out[0] = decay_rate * left_ref[0] + (1.0 - decay_rate) * left
        right = lax.dot_general(cols, ref[...], (((0,), (0,)), ((), ())), preferred_element_type=jnp.float32)
        right_out[0] = decay_rate * right_ref[0] + (1.0 - decay_rate) * right.T

    @pl.when(filled & (slot == (rep & 1)))
    def _():
        update(grad_ref)

    @pl.when(filled & (slot != (rep & 1)))
    def _():
        update(other_ref)

    @pl.when(jnp.logical_not(filled))
    def _():
        left_out[...] = left_ref[...]
        right_out[...] = right_ref[...]


def stats(table, where, grad, other, left, right):
    whole = pl.BlockSpec(grad.shape, lambda i, *_: (0, 0))
    one = pl.BlockSpec((1,) + left.shape[1:], lambda i, *_: (i, 0, 0))
    return pl.pallas_call(
        stats_kernel,
        grid_spec=pltpu.PrefetchScalarGridSpec(
            num_scalar_prefetch=2,
            grid=(2,),
            in_specs=[whole, whole, one, one],
            out_specs=[one, one],
        ),
        out_shape=[jax.ShapeDtypeStruct(left.shape, left.dtype)] * 2,
        compiler_params=pltpu.CompilerParams(vmem_limit_bytes=28 * 1024 * 1024),
    )(table, where, grad, other, left, right)


def left_kernel(both, where_ref, left_ref, near_ref, *parts):
    me, side = where_ref[0], where_ref[1] & 1
    for j in range(len(parts)):
        rows = pl.ds(pl.multiple_of(((me >> 1) ^ j) * both, both), both)
        parts[j][0] = left_ref[side, rows, :]
        parts[j][1] = near_ref[rows, :]


def pack_kernel(owners, where_ref, *refs):
    for k in range(owners):
        refs[-1][k] = refs[k][1 - (where_ref[1] & 1)]


def collect_kernel(owners, table_ref, where_ref, *refs):
    pieces, beside_ref, out_ref = refs[:-2], refs[-2], refs[-1]
    me, side = where_ref[0], where_ref[1] & 1
    for k in range(owners):
        block = table_ref[(me ^ k) * 2 + side]

        @pl.when(block >= 0)
        def _(k=k, block=block):
            out_ref[block] = pieces[k][side]

        beside = table_ref[(me ^ k) * 2 + 1 - side]

        @pl.when(beside >= 0)
        def _(k=k, beside=beside):
            out_ref[beside] = beside_ref[k]


def call(kernel, scalars, out_shape, ins, scratch=()):
    vmem = pl.BlockSpec(memory_space=pltpu.VMEM)
    smem = pl.BlockSpec(memory_space=pltpu.SMEM)
    return pl.pallas_call(
        kernel,
        out_shape=out_shape,
        in_specs=[smem] * len(scalars) + [vmem] * len(ins),
        out_specs=jax.tree.map(lambda _: vmem, out_shape),
        scratch_shapes=scratch,
        compiler_params=pltpu.CompilerParams(vmem_limit_bytes=24 * 1024 * 1024),
    )(*scalars, *ins)


def on_device(owners, quarters, partial_grad, owner_table, left_stat, right_stat, left_root, right_root):
    grad = partial_grad[0]
    me, rep = lax.axis_index("fsdp"), lax.axis_index("rep")
    side = rep & 1
    slots, order, width = left_stat.shape[1:]
    assert slots == 2
    rows = grad.shape[1]
    table = owner_table.reshape(-1)
    where = jnp.stack([me, rep]).astype(jnp.int32)
    bf16 = lambda *shape: jax.ShapeDtypeStruct(shape, jnp.bfloat16)

    def swap(x, bits):
        return lax.ppermute(x, "rep", [(r, r ^ bits) for r in range(quarters)])

    def give(x, k):
        return lax.ppermute(x, "fsdp", [(f, f ^ k) for f in range(owners)])

    def slot(x, s):
        return lax.dynamic_index_in_dim(x, s, 0, keepdims=False)

    near = swap(grad, 1)
    part = lax.dynamic_slice_in_dim(grad, (rep ^ 2) * width, width, 2)
    halves = call(pair_kernel, (where,), (bf16(grad.shape[0], rows, width // 2),) * 2, (part, near))
    across = [swap(halves[p], 2) for p in range(2)]
    base = jax.ShapeDtypeStruct((2, *part.shape), jnp.float32)
    base = call(base_kernel, (where,), base, (grad, near))
    beside = [swap(across[p], 1) for p in range(2)]
    left, right = left_root[0], right_root[0]
    left_near = swap(slot(left, 1 - side), 1)
    right_near = swap(slot(right, 1 - side), 1)
    left_parts = call(
        functools.partial(left_kernel, 2 * rows),
        (where,),
        (bf16(2, 2 * rows, width),) * (owners // 2),
        (left, left_near),
    )
    half = owners // 2
    piece, split = bf16(2, rows, width), bf16(2, rows, width // 2)
    early = call(
        functools.partial(route_kernel, [(k, (0,)) for k in range(half, owners)]),
        (table, where),
        (split,) * half,
        (base, across[0], beside[0]),
    )
    pieces = call(
        functools.partial(route_kernel, [(k, (0, 1)) for k in range(half)] + [(k, (1,)) for k in range(half, owners)]),
        (table, where),
        (piece,) * half + (split,) * half,
        (base, across[0], beside[0], across[1], beside[1]),
    )
    early = [give(early[k - half], k) for k in range(half, owners)]
    joined = call(join_kernel, (), bf16(half, 2, rows, width // 2), early)
    joined = swap(joined, 2)
    gathered = []
    for k in range(owners):
        own = give(pieces[k], k) if k else pieces[k]
        gathered += [own, swap(own, 2)]
    gradient, product = call(
        functools.partial(product_kernel, owners),
        (where,),
        (bf16(order, order), bf16(2, order, width)),
        (*gathered, *early, joined, right, right_near),
    )
    returned = {}
    for j in reversed(range(owners // 2)):
        part = left_parts[j]
        far = swap(part, 2)
        same, odd = call(apply_kernel, (where,), (bf16(2, rows, width),) * 2, (part, far, product))
        returned[2 * j + 1] = give(odd, 2 * j + 1)
        returned[2 * j] = give(same, 2 * j) if j else same
    other = swap(gradient, 1)
    left_next, right_next = stats(table, where, gradient, other, left_stat[0], right_stat[0])
    returned[0], left_next, right_next = lax.optimization_barrier((returned[0], left_next, right_next))
    returned = [returned[k] for k in range(owners)]
    packed = call(functools.partial(pack_kernel, owners), (where,), bf16(owners, rows, width), returned)
    update = call(
        functools.partial(collect_kernel, owners),
        (table, where),
        bf16(grad.shape[0], rows, width),
        (*returned, swap(packed, 1)),
    )
    return left_next[None], right_next[None], update


def solution(mesh):
    owners, quarters = mesh.shape["fsdp"], mesh.shape["rep"]
    assert quarters == 4 and owners & (owners - 1) == 0
    stat = P("fsdp", None, None, "rep")

    def body(*args):
        return on_device(owners, quarters, *args)

    return jax.shard_map(
        body,
        mesh=mesh,
        in_specs=(P("rep", None, "fsdp", None), P(), stat, stat, stat, stat),
        out_specs=(stat, stat, P(None, "fsdp", "rep")),
        check_vma=False,
    )
```

```python
import functools

import jax
import jax.numpy as jnp
from jax import lax
from jax.experimental import pallas as pl
from jax.experimental.pallas import tpu as pltpu
from jax.sharding import PartitionSpec as P


decay_rate = 0.99


def first_pair_kernel(mine_ref, near_ref, out_ref):
    out_ref[...] = (mine_ref[...].astype(jnp.float32) + near_ref[...].astype(jnp.float32)).astype(jnp.bfloat16)


def second_pair_kernel(where_ref, grad_ref, near_ref, out_ref, base_ref):
    step = out_ref.shape[2]
    cols = pl.ds(pl.multiple_of((where_ref[1] ^ 2) * 2 * step + step, step), step)
    total = grad_ref[:, :, cols].astype(jnp.float32) + near_ref[:, :, cols].astype(jnp.float32)
    out_ref[...] = total.astype(jnp.bfloat16)
    for q in range(2):
        cols = pl.ds(pl.multiple_of((where_ref[1] ^ q) * 2 * step, 2 * step), 2 * step)
        base_ref[q] = grad_ref[:, :, cols].astype(jnp.float32) + near_ref[:, :, cols].astype(jnp.float32)


def route_kernel(wanted, table_ref, where_ref, base_ref, *refs):
    sums, pieces = refs[: len(refs) - len(wanted)], refs[len(refs) - len(wanted) :]
    me, side = where_ref[0], where_ref[1] & 1
    step = sums[0].shape[2]
    for (k, parts), piece in zip(wanted, pieces):
        block = table_ref[side, me ^ k]

        @pl.when(block >= 0)
        def _(parts=parts, piece=piece, block=block):
            for n, p in enumerate(parts):
                for q in range(2):
                    total = base_ref[q, block, :, p * step : (p + 1) * step]
                    far_ref = sums[2 * p + q] if len(sums) > 2 else sums[q]
                    total = total + far_ref[block].astype(jnp.float32)
                    piece[side ^ q, :, n * step : (n + 1) * step] = total.astype(jnp.bfloat16)

        @pl.when(block < 0)
        def _(piece=piece):
            piece[...] = jnp.zeros(piece.shape, jnp.bfloat16)


def join_kernel(*refs):
    for n in range(len(refs) - 1):
        refs[-1][n] = refs[n][...]


def product_kernel(owners, where_ref, *refs):
    joined_ref, right_ref, beside_ref, grad_ref, prod_ref = refs[-5:]
    half = owners // 2
    rows, width = refs[0].shape[1:]
    step = width // 2
    me, side, place = where_ref[0], where_ref[1] & 1, where_ref[1] >> 1
    for k in range(owners):
        first = pl.ds(pl.multiple_of((me ^ k) * rows, rows), rows)
        for i in range(2):
            for q in range(2):
                col = pl.multiple_of(((place ^ i) * 2 + q) * width, width)
                if k < half:
                    grad_ref[first, pl.ds(col, width)] = refs[2 * k + i][q]
                else:
                    early = joined_ref[k - half, q] if i else refs[2 * owners + k - half][q]
                    grad_ref[first, pl.ds(col, step)] = early
                    grad_ref[first, pl.ds(pl.multiple_of(col + step, step), step)] = refs[2 * k + i][q]
    for i, right in enumerate((right_ref[side], beside_ref[...])):
        prod_ref[i] = jnp.dot(grad_ref[...], right, preferred_element_type=jnp.float32).astype(jnp.bfloat16)


def apply_kernel(where_ref, near_ref, far_ref, prod_ref, even_ref, odd_ref):
    _, both, width = near_ref.shape
    rows = both // 2
    me, rep = where_ref[0], where_ref[1]
    side = rep & 1
    swapped = (me & 1) == 1
    for i in range(2):
        total = None
        for q in range(4):
            band = pl.ds(pl.multiple_of((rep ^ q) * width, width), width)
            ref = far_ref if q & 2 else near_ref
            term = jnp.dot(ref[q & 1], prod_ref[i, band, :], preferred_element_type=jnp.float32)
            total = term if total is None else total + term
        total = total.astype(jnp.bfloat16)
        even_ref[side ^ i] = jnp.where(swapped, total[rows:], total[:rows])
        odd_ref[side ^ i] = jnp.where(swapped, total[:rows], total[rows:])


def product_apply_kernel(owners, where_ref, near_ref, far_ref, *refs):
    product_kernel(owners, where_ref, *refs[:-2])
    apply_kernel(where_ref, near_ref, far_ref, *refs[-3:])


def stats_kernel(table_ref, where_ref, grad_ref, other_ref, left_ref, right_ref, left_out, right_out):
    me, rep = where_ref[0], where_ref[1]
    _, _, width = left_ref.shape
    slot = pl.program_id(0)
    filled = table_ref[slot, me] >= 0
    share = pl.ds(pl.multiple_of(rep * width, width), width)

    def update(ref):
        rows, cols = ref[share, :], ref[:, share]
        left = lax.dot_general(ref[...], rows, (((1,), (1,)), ((), ())), preferred_element_type=jnp.float32)
        left_out[0] = decay_rate * left_ref[0] + (1.0 - decay_rate) * left
        right = lax.dot_general(cols, ref[...], (((0,), (0,)), ((), ())), preferred_element_type=jnp.float32)
        right_out[0] = decay_rate * right_ref[0] + (1.0 - decay_rate) * right.T

    @pl.when(filled & (slot == (rep & 1)))
    def _():
        update(grad_ref)

    @pl.when(filled & (slot != (rep & 1)))
    def _():
        update(other_ref)

    @pl.when(jnp.logical_not(filled))
    def _():
        left_out[...] = left_ref[...]
        right_out[...] = right_ref[...]


def stats(table, where, grad, other, left, right):
    whole = pl.BlockSpec(grad.shape, lambda i, *_: (0, 0))
    one = pl.BlockSpec((1,) + left.shape[1:], lambda i, *_: (i, 0, 0))
    return pl.pallas_call(
        stats_kernel,
        grid_spec=pltpu.PrefetchScalarGridSpec(
            num_scalar_prefetch=2,
            grid=(2,),
            in_specs=[whole, whole, one, one],
            out_specs=[one, one],
        ),
        out_shape=[jax.ShapeDtypeStruct(left.shape, left.dtype)] * 2,
        compiler_params=pltpu.CompilerParams(vmem_limit_bytes=28 * 1024 * 1024),
    )(table, where, grad, other, left, right)


def left_kernel(pairs, where_ref, left_ref, near_ref, *parts):
    both = parts[0].shape[1]
    me, side = where_ref[0], where_ref[1] & 1
    for j, part in zip(pairs, parts):
        rows = pl.ds(pl.multiple_of(((me >> 1) ^ j) * both, both), both)
        part[0] = left_ref[side, rows, :]
        part[1] = near_ref[rows, :]


def pack_kernel(where_ref, *refs):
    for n in range(len(refs) - 1):
        refs[-1][n] = refs[n][1 - (where_ref[1] & 1)]


def collect_kernel(owners, packed, late, table_ref, where_ref, *refs):
    pieces, out_ref = refs[:owners], refs[-1]
    me, side = where_ref[0], where_ref[1] & 1
    for k in range(owners):
        block = table_ref[side, me ^ k]

        @pl.when(block >= 0)
        def _(k=k, block=block):
            out_ref[block] = pieces[k][side]

        other = table_ref[1 - side, me ^ k]

        @pl.when(other >= 0)
        def _(k=k, other=other):
            if k in late:
                out_ref[other] = refs[owners + 1 + late.index(k)][side]
            else:
                out_ref[other] = refs[owners][packed.index(k)]


def call(kernel, scalars, out_shape, ins, limit=8):
    vmem = pl.BlockSpec(memory_space=pltpu.VMEM)
    smem = pl.BlockSpec(memory_space=pltpu.SMEM)
    return pl.pallas_call(
        kernel,
        out_shape=out_shape,
        in_specs=[smem] * len(scalars) + [vmem] * len(ins),
        out_specs=jax.tree.map(lambda _: vmem, out_shape),
        compiler_params=pltpu.CompilerParams(vmem_limit_bytes=limit * 1024 * 1024),
    )(*scalars, *ins)


def on_device(owners, quarters, partial_grad, owner_table, left_stat, right_stat, left_root, right_root):
    grad = partial_grad[0]
    me, rep = lax.axis_index("fsdp"), lax.axis_index("rep")
    side = rep & 1
    slots, order, width = left_stat.shape[1:]
    assert slots == 2
    rows = grad.shape[1]
    table = owner_table.T
    where = jnp.stack([me, rep]).astype(jnp.int32)
    bf16 = lambda *shape: jax.ShapeDtypeStruct(shape, jnp.bfloat16)

    def swap(x, bits):
        return lax.ppermute(x, "rep", [(r, r ^ bits) for r in range(quarters)])

    def give(x, k):
        return lax.ppermute(x, "fsdp", [(f, f ^ k) for f in range(owners)])

    def slot(x, s):
        return lax.dynamic_index_in_dim(x, s, 0, keepdims=False)

    def cut(q):
        return lax.dynamic_slice_in_dim(grad, q * width, width // 2, 2)

    half = bf16(grad.shape[0], rows, width // 2)
    lead = swap(cut(rep ^ 3), 1)
    near = swap(grad, 1)
    first = call(first_pair_kernel, (), half, (cut(rep ^ 2), lead))
    base = jax.ShapeDtypeStruct((2, grad.shape[0], rows, width), jnp.float32)
    second, base = call(second_pair_kernel, (where,), (half, base), (grad, near))
    across = [swap(first, 2), swap(second, 2)]
    beside = [swap(across[p], 1) for p in range(2)]
    left, right = left_root[0], right_root[0]
    left_near = swap(slot(left, 1 - side), 1)
    right_near = swap(slot(right, 1 - side), 1)
    half = owners // 2
    left_parts = {}
    for pairs in ([half - 1, half - 2], list(range(half - 2))):
        parts = call(
            functools.partial(left_kernel, pairs),
            (where,),
            (bf16(2, 2 * rows, width),) * len(pairs),
            (left, left_near),
        )
        left_parts.update(zip(pairs, parts))
    piece, split = bf16(2, rows, width), bf16(2, rows, width // 2)
    early = call(
        functools.partial(route_kernel, [(k, (0,)) for k in range(half, owners)]),
        (table, where),
        (split,) * half,
        (base, across[0], beside[0]),
    )
    pieces = call(
        functools.partial(route_kernel, [(k, (0, 1)) for k in range(half)] + [(k, (1,)) for k in range(half, owners)]),
        (table, where),
        (piece,) * half + (split,) * half,
        (base, across[0], beside[0], across[1], beside[1]),
    )
    early = [give(early[k - half], k) for k in range(half, owners)]
    joined = call(join_kernel, (), bf16(half, 2, rows, width // 2), early)
    joined = swap(joined, 2)
    gathered = []
    for k in range(owners):
        own = give(pieces[k], k) if k else pieces[k]
        gathered += [own, swap(own, 2)]
    returned = {}
    result = bf16(2, rows, width)
    for j in reversed(range(half)):
        part = left_parts[j]
        far = swap(part, 2)
        if j == half - 1:
            gradient, product, same, odd = call(
                functools.partial(product_apply_kernel, owners),
                (where,),
                (bf16(order, order), bf16(2, order, width), result, result),
                (part, far, *gathered, *early, joined, right, right_near),
                12,
            )
        else:
            same, odd = call(apply_kernel, (where,), (result, result), (part, far, product))
        returned[2 * j + 1] = give(odd, 2 * j + 1)
        returned[2 * j] = give(same, 2 * j) if j else same
    other = swap(gradient, 1)
    left_next, right_next = stats(table, where, gradient, other, left_stat[0], right_stat[0])
    late = [2, 3, half]
    packed = [k for k in range(owners) if k not in late]
    beside = [call(pack_kernel, (where,), bf16(len(packed), rows, width), [returned[k] for k in packed])]
    beside = [swap(beside[0], 1)] + [swap(returned[k], 1) for k in late]
    update = call(
        functools.partial(collect_kernel, owners, packed, late),
        (table, where),
        bf16(grad.shape[0], rows, width),
        (*(returned[k] for k in range(owners)), *beside),
    )
    return left_next[None], right_next[None], update


def solution(mesh):
    owners, quarters = mesh.shape["fsdp"], mesh.shape["rep"]
    assert quarters == 4 and owners & (owners - 1) == 0
    stat = P("fsdp", None, None, "rep")

    def body(*args):
        return on_device(owners, quarters, *args)

    return jax.shard_map(
        body,
        mesh=mesh,
        in_specs=(P("rep", None, "fsdp", None), P(), stat, stat, stat, stat),
        out_specs=(stat, stat, P(None, "fsdp", "rep")),
        check_vma=False,
    )
```
